32 devices in a mesh: dp: 4 (over y, x), expert: 8 (over z, core).
Axes of the slice: x: 2, y: 2, z: 4, core: 2. Of those that a mesh axis runs over, the one named last changes fastest.
Arguments:
- residual: bfloat16 [2048, 1024], P(('dp', 'expert')), parts along dimension 0, may hold values from -6 to 6
- expert_ids: int32 [2048, 8], P(('dp', 'expert')), parts along dimension 0, may hold values from 0 to 63, all different within a row; in each aligned block of 64 rows (0 to 63, 64 to 127, ...) at most 12 rows name the same one
- route_weights: float32 [2048, 8], P(('dp', 'expert')), parts along dimension 0, may hold values from 0.05 to 0.5
- expert_out: bfloat16 [24576, 1024], P(('dp', 'expert')), parts along dimension 0, may hold values from -6 to 6
Outputs:
- mixed: bfloat16 [2048, 1024], P(('dp', 'expert')), parts along dimension 0
- expert_load: float32 [256], P('dp'), parts along dimension 0
The draws below stay inside these ranges and needn't reach their ends.
There are 4 independent parts, one for each index of `dp`. The reference program is written for one: setup_inputs(seed, part) draws one part's arguments, and reference() takes and returns one part's arrays. A program takes and returns all parts, laid end to end along the dimension named above; each array names one. Nothing has to cross between parts.
Inputs may be any that keep to these rules, and one draw needn't show every extreme that they name: `expert_ids`: each row names 8 different experts. Within the rows of one device no expert is named by more than 12 rows, and in some devices' rows an expert is named by exactly 12.
All inputs are finite; a program needn't handle non-finite values.
Results may differ from the reference program's by a relative error of at most 0.001.
Values may be sent and summed in bfloat16 or wider, within the bound.
A program may use at most 64 MiB of HBM per device.

```python
import math
import jax
import jax.numpy as jnp
import numpy as np
from jax import lax

D = 1024
EXPERTS = 64
TOP = 8
TOK_DEV = 64
CAP_E = 12
TOKENS = 512
SLOT_ROWS = 6144
N_EXPERT = 8


def steps_of(key, shape, shards, smallest, top_value):
    def one(dim, shards_of):
        heights = jax.random.uniform(jax.random.fold_in(jax.random.fold_in(key, 6), dim), (shards_of,), jnp.float32, smallest / len(shards), top_value / len(shards))
        return jnp.repeat(jnp.exp(heights), shape[dim] // shards_of).reshape((-1,) + (1,) * (len(shape) - dim - 1))

    loudness = one(*shards[0])
    for cut in shards[1:]:
        loudness = loudness * one(*cut)
    return loudness


def shared_out(stream_key, own, number, rows, count, top, bound, slope):
    sequence = jax.random.permutation(stream_key, count)
    packed, ordinary = portions_of(count, rows * top, bound, slope, True), portions_of(count, rows * top, bound, slope, False)
    places = jnp.arange(count)

    def named(tallies, turn):
        used = int((tallies > 0).sum())
        fixed = max(1, used // 4)
        moved = fixed + (places - fixed + turn * (used - fixed)) % max(1, count - fixed)
        return jnp.zeros((count,), jnp.int32).at[sequence[jnp.where(places < fixed, places, moved)]].set(jnp.asarray(tallies, jnp.int32))

    tallies = jnp.where(number % 4 == 0, named(packed, number // 4), named(ordinary, number - number // 4 - 1))
    mixed = jax.random.permutation(jax.random.fold_in(own, 3), count)
    donor, taker = mixed[0:count // 2 * 2:2], mixed[1:count // 2 * 2:2]
    room = jnp.minimum(tallies[donor] - 1, bound - tallies[taker]) // 2
    room = jnp.where((donor == sequence[0]) | (taker == sequence[0]) | (tallies[taker] == 0), 0, jnp.maximum(room, 0))
    moved = jax.random.randint(jax.random.fold_in(own, 4), (count // 2,), 0, 1 << 20) % (room + 1)
    tallies = tallies.at[donor].add(-moved).at[taker].add(moved)
    members = jnp.searchsorted(jnp.cumsum(tallies), jnp.arange(rows * top), side="right").astype(jnp.int32)
    table = members.reshape(top, rows).T
    table = table[jax.random.permutation(jax.random.fold_in(own, 1), rows)]
    turn = jax.random.randint(jax.random.fold_in(own, 2), (rows, 1), 0, top)
    return jnp.take_along_axis(table, (jnp.arange(top)[None, :] + turn) % top, axis=1)


def portions_of(amount, total, most, slope, full):
    weights = [(1 << 20) // math.isqrt(rank ** slope) + 1 for rank in range(1, amount + 1)]
    largest = most if full else min(most, max(-(-total // amount), total * weights[0] // sum(weights)))
    least = 1 if total - largest >= amount - 1 else 0
    counts, spare = [largest] + [least] * (amount - 1), total - largest - least * (amount - 1)
    while spare > 0:
        candidates = [i for i in range(1, amount) if counts[i] < largest] or [i for i in range(1, amount) if counts[i] < most]
        pool, left = sum([weights[i] for i in candidates]), spare
        for i in candidates:
            addition = min(most - counts[i], max(1, left * weights[i] // pool), spare)
            counts[i] = counts[i] + addition
            spare = spare - addition
    return np.array(counts)


def bell_draw(stream_key, shape, scale, most, split=(), kind=jnp.bfloat16):
    entries = jax.random.normal(stream_key, shape, jnp.float32) * scale
    if len(split) > 0:
        entries = steps_of(stream_key, shape, split, -0.22, 0.18) * entries
    return jnp.clip(entries, min=-most, max=most).astype(kind)


def setup_inputs(seed: int = 0, part: int = 0) -> dict:
    streams_of = jax.random.split(jax.random.key(seed), 5)
    part_splits = jax.random.split(jax.random.fold_in(streams_of[4], part), 5)
    residual = bell_draw(part_splits[0], (TOKENS, D), 1.0, 6.0, ((0, 8),))
    expert_ids_keys = jax.random.split(jax.random.fold_in(part_splits[1], 1), TOKENS // TOK_DEV)
    expert_ids_turns = jax.random.permutation(jax.random.fold_in(part_splits[1], 3), TOKENS // TOK_DEV)
    expert_ids = jax.vmap(lambda own, number: shared_out(jax.random.fold_in(part_splits[1], 2), own, number, TOK_DEV, EXPERTS, TOP, CAP_E, 2))(expert_ids_keys, expert_ids_turns).reshape((TOKENS, TOP))
    route_weights = jnp.clip(jnp.exp(math.log(0.5) - 2.3025851 * jax.random.uniform(part_splits[2], (TOKENS, TOP), jnp.float32) ** steps_of(part_splits[2], (TOKENS, TOP), ((0, 8),), -0.2, 0.2)), 0.05, 0.5)
    expert_out = bell_draw(part_splits[3], (SLOT_ROWS, D), 1.0, 6.0, ((0, 8),))
    return {"residual": residual, "expert_ids": expert_ids, "route_weights": route_weights, "expert_out": expert_out}


def reference(residual, expert_ids, route_weights, expert_out):
    per_peer = EXPERTS * CAP_E // N_EXPERT
    held_rows = EXPERTS * CAP_E
    catalog = jnp.arange(EXPERTS, dtype=jnp.int32)

    def one_owner(owner):
        routes = lax.dynamic_slice_in_dim(expert_ids, owner * TOK_DEV, TOK_DEV, 0).reshape(-1)
        onehot = (routes[:, None] == catalog[None, :]).astype(jnp.int32)
        earlier = jnp.cumsum(onehot, axis=0, dtype=jnp.int32) - onehot
        slots = jnp.sum(earlier * onehot, axis=1, dtype=jnp.int32)
        position = routes * CAP_E + slots
        rows = (position // per_peer) * held_rows + owner * per_peer + position % per_peer
        picked = jnp.take(expert_out, rows.astype(jnp.int32), axis=0).reshape(TOK_DEV, TOP, D)
        weights = lax.dynamic_slice_in_dim(route_weights, owner * TOK_DEV, TOK_DEV, 0)
        total = lax.dynamic_slice_in_dim(residual, owner * TOK_DEV, TOK_DEV, 0).astype(jnp.float32)
        for choice_index in range(TOP):
            total = total + weights[:, choice_index:choice_index + 1] * picked[:, choice_index].astype(jnp.float32)
        return total.astype(jnp.bfloat16), jnp.sum(onehot, axis=0, dtype=jnp.int32)

    mixed, loads = lax.map(one_owner, jnp.arange(N_EXPERT, dtype=jnp.int32))
    return mixed.reshape(TOKENS, D), jnp.sum(loads, axis=0, dtype=jnp.int32).astype(jnp.float32)
```

```python
import functools
import jax
import jax.numpy as jnp
from jax import lax
from jax.experimental import pallas as pl
from jax.experimental.pallas import tpu as pltpu
from jax.sharding import PartitionSpec as P

EXPERTS = 64
CORES = 2
VMEM_BUDGET = 24 * 1024 * 1024


def dot(a, b, dims=(((1,), (0,)), ((), ()))):
    return lax.dot_general(a, b, dims, preferred_element_type=jnp.float32)


def combine_kernel(
    chips, capacity,
    ids_ref, weights_ref, residual_ref, rows_hbm,
    mixed_ref, load_ref,
    raw, ids_all, weights_all, partial, arrived, own_sum, counts, counts_in,
    local_sem, raw_send, raw_recv, ids_send, ids_recv, w_send, w_recv,
    out_send, out_recv, load_sems,
):
    me = lax.axis_index("expert")
    chip, core = me // CORES, me % CORES
    other = 1 - core
    partner = {"expert": chip * CORES + other}
    tokens, width = residual_ref.shape
    fanout = ids_ref.shape[0]
    per_peer = rows_hbm.shape[1]
    held = CORES * per_peer
    local_experts = held // capacity

    def peer(step):
        return lax.rem(chip + step, chips)

    def device(step):
        return {"expert": peer(step) * CORES + core}

    barrier = pltpu.get_barrier_semaphore()
    pl.semaphore_signal(barrier, inc=1, device_id=partner)
    for step in range(1, chips):
        pl.semaphore_signal(barrier, inc=1, device_id=device(step))

    local = []
    for j in range(chips):
        copy = pltpu.make_async_copy(rows_hbm.at[j * CORES + core], raw.at[j, core], local_sem.at[j])
        copy.start()
        local.append(copy)
    pl.semaphore_wait(barrier, chips)

    routing = []
    for step in range(1, chips):
        a = pltpu.make_async_remote_copy(
            ids_ref, ids_all.at[step], ids_send.at[step], ids_recv.at[step], device_id=device(step))
        b = pltpu.make_async_remote_copy(
            weights_ref, weights_all.at[step], w_send.at[step], w_recv.at[step], device_id=device(step))
        a.start()
        b.start()
        routing.append((a, b))
    rows = []
    for j in range(chips):
        copy = pltpu.make_async_remote_copy(
            rows_hbm.at[j * CORES + other], raw.at[j, core], raw_send.at[j], raw_recv.at[j],
            device_id=partner)
        copy.start()
        rows.append(copy)

    before = (lax.broadcasted_iota(jnp.int32, (tokens, tokens), 0)
              < lax.broadcasted_iota(jnp.int32, (tokens, tokens), 1)).astype(jnp.float32).astype(jnp.bfloat16)
    place = lax.broadcasted_iota(jnp.int32, (held, local_experts), 0)
    which = lax.broadcasted_iota(jnp.int32, (held, local_experts), 1)
    low = which * capacity
    spread = ((place >= low) & (place < low + capacity)).astype(jnp.float32).astype(jnp.bfloat16)
    wanted = (lax.broadcasted_iota(jnp.int32, (held, tokens), 0) % capacity).astype(jnp.float32)
    expert = lax.broadcasted_iota(jnp.int32, (local_experts, tokens), 0) + chip * local_experts

    def select(ids, weights):
        chosen = jnp.zeros((local_experts, tokens), jnp.float32)
        weight = jnp.zeros((local_experts, tokens), jnp.float32)
        for k in range(fanout):
            hit = ids[k:k + 1, :] == expert
            chosen = jnp.where(hit, 1.0, chosen)
            weight = jnp.where(hit, weights[k:k + 1, :], weight)
        slot = dot(chosen.astype(jnp.bfloat16), before)
        slot = jnp.where(chosen > 0, slot, -1.0)
        keep = dot(spread, slot.astype(jnp.bfloat16)) == wanted
        pieces = []
        rest = weight
        for _ in range(3):
            piece = rest.astype(jnp.bfloat16)
            rest = rest - piece.astype(jnp.float32)
            pieces.append(jnp.where(keep, dot(spread, piece), 0.0))
        return pieces

    def combine(pieces, block):
        total = None
        for piece in pieces:
            part = dot(jnp.transpose(piece).astype(jnp.bfloat16), block)
            total = part if total is None else total + part
        return total

    sends = []
    order = [chips // 2] + [s for s in range(1, chips) if s != chips // 2]
    for j in range(chips):
        local[j].wait()
        rows[j].wait()
    for step in order:
        routing[step - 1][0].wait()
        routing[step - 1][1].wait()
        j = lax.rem(chip + chips - step, chips)
        pieces = select(ids_all[step], weights_all[step])
        partial[step] = combine(pieces, raw[j].reshape(held, width))
        copy = pltpu.make_async_remote_copy(
            partial.at[step], arrived.at[step], out_send.at[step], out_recv.at[step],
            device_id=device(chips - step))
        copy.start()
        sends.append(copy)

    own_sum[...] = combine(select(ids_ref[...], weights_ref[...]), raw[chip].reshape(held, width))

    every = lax.broadcasted_iota(jnp.int32, (EXPERTS, tokens), 0)
    seen = jnp.zeros((EXPERTS, tokens), jnp.float32)
    for step in range(chips):
        ids = ids_ref[...] if step == 0 else ids_all[step]
        for k in range(fanout):
            seen = seen + jnp.where(ids[k:k + 1, :] == every, 1.0, 0.0)
    ones = jnp.ones((8, tokens), jnp.float32).astype(jnp.bfloat16)
    counts[...] = dot(ones, seen.astype(jnp.bfloat16), (((1,), (1,)), ((), ())))
    tally = pltpu.make_async_remote_copy(
        counts, counts_in, load_sems.at[0], load_sems.at[1], device_id=partner)
    tally.start()

    own_sum[...] = own_sum[...] + residual_ref[...].astype(jnp.float32)
    tally.wait()
    load_ref[...] = (counts[...] + counts_in[...])[0:1, :]
    for n, step in enumerate(order):
        sends[n].wait()
        own_sum[...] = own_sum[...] + arrived[step]
    mixed_ref[...] = own_sum[...].astype(jnp.bfloat16)


def fused(chips, residual, expert_ids, route_weights, expert_out):
    peers = chips * CORES
    tokens, width = residual.shape
    fanout = expert_ids.shape[1]
    per_peer = expert_out.shape[0] // peers
    capacity = expert_out.shape[0] // EXPERTS
    vmem = pl.BlockSpec(memory_space=pltpu.VMEM)
    dma = pltpu.SemaphoreType.DMA
    mixed, load = pl.pallas_call(
        functools.partial(combine_kernel, chips, capacity),
        out_shape=(
            jax.ShapeDtypeStruct((tokens, width), jnp.bfloat16),
            jax.ShapeDtypeStruct((1, EXPERTS), jnp.float32),
        ),
        in_specs=[vmem, vmem, vmem, pl.BlockSpec(memory_space=pl.ANY)],
        out_specs=(vmem, vmem),
        scratch_shapes=[
            pltpu.VMEM((chips, CORES, per_peer, width), jnp.bfloat16),
            pltpu.VMEM((chips, fanout, tokens), jnp.int32),
            pltpu.VMEM((chips, fanout, tokens), jnp.float32),
            pltpu.VMEM((chips, tokens, width), jnp.float32),
            pltpu.VMEM((chips, tokens, width), jnp.float32),
            pltpu.VMEM((tokens, width), jnp.float32),
            pltpu.VMEM((8, EXPERTS), jnp.float32),
            pltpu.VMEM((8, EXPERTS), jnp.float32),
        ] + [dma((chips,))] * 9 + [dma((2,))],
        compiler_params=pltpu.CompilerParams(collective_id=0, has_side_effects=True),
    )(expert_ids.T, route_weights.T, residual, expert_out.reshape(peers, per_peer, width))
    return mixed, load.reshape(EXPERTS)


def general(residual, expert_ids, route_weights, expert_out):
    peers = lax.axis_size("expert")
    per_peer = expert_out.shape[0] // peers
    width = residual.shape[1]
    tokens_here = expert_ids.shape[0]
    fanout = expert_ids.shape[1]
    capacity = expert_out.shape[0] // EXPERTS
    routes = expert_ids.reshape(-1)
    onehot = (routes[:, None] == jnp.arange(EXPERTS, dtype=jnp.int32)[None, :]).astype(jnp.int32)
    earlier = jnp.cumsum(onehot, axis=0, dtype=jnp.int32) - onehot
    slots = jnp.sum(earlier * onehot, axis=1, dtype=jnp.int32)
    source_rows = routes * capacity + slots
    load_totals = lax.psum(jnp.sum(onehot, axis=0).astype(jnp.float32), "expert")
    blocks = expert_out.reshape(peers, per_peer, width)
    arrived = lax.all_to_all(blocks, "expert", split_axis=0, concat_axis=0, tiled=True)
    picked = jnp.take(arrived.reshape(peers * per_peer, width), source_rows, axis=0)
    picked = picked.reshape(tokens_here, fanout, width)
    total = residual.astype(jnp.float32)
    for k in range(fanout):
        total = total + route_weights[:, k, None] * picked[:, k].astype(jnp.float32)
    return total.astype(jnp.bfloat16), load_totals


def solution(mesh):
    peers = mesh.shape["expert"]

    def per_device(residual, expert_ids, route_weights, expert_out):
        tokens, width = residual.shape
        slots = expert_out.shape[0]
        capacity, per_peer = slots // EXPERTS, slots // peers
        chips = peers // CORES
        needed = slots * width * 2 + (2 * chips + 4) * tokens * width * 4
        fits = (
            peers % CORES == 0 and chips > 1 and slots % EXPERTS == 0
            and per_peer % capacity == 0 and per_peer % 16 == 0 and needed <= VMEM_BUDGET
        )
        if fits:
            return fused(chips, residual, expert_ids, route_weights, expert_out)
        return general(residual, expert_ids, route_weights, expert_out)

    split = P(("dp", "expert"), None)
    return jax.shard_map(
        per_device,
        mesh=mesh,
        in_specs=(split,) * 4,
        out_specs=(split, P("dp")),
        check_vma=False,
    )
```

```python
import functools
import jax
import jax.numpy as jnp
from jax import lax
from jax.experimental import pallas as pl
from jax.experimental.pallas import tpu as pltpu
from jax.sharding import PartitionSpec as P

EXPERTS = 64
CORES = 2
VMEM_BUDGET = 24 * 1024 * 1024


def dot(a, b, dims=(((1,), (0,)), ((), ()))):
    return lax.dot_general(a, b, dims, preferred_element_type=jnp.float32)


LEVELS = 32767.0


def encode(x):
    top = jnp.maximum(jnp.max(jnp.abs(x), axis=1, keepdims=True), 1e-30)
    code = jnp.round(x * (LEVELS / top)).astype(jnp.int32).astype(jnp.int16)
    scale = jnp.transpose(jnp.broadcast_to(top * (1.0 / LEVELS), (x.shape[0], 128)))[0:8, :]
    return code, scale


def decode(code, scale):
    column = jnp.transpose(jnp.broadcast_to(scale[0:1, :], (128, scale.shape[1])))[:, 0:1]
    return code.astype(jnp.int32).astype(jnp.float32) * column


def combine_kernel(
    chips, capacity,
    ids_ref, weights_ref, residual_ref, rows_hbm,
    mixed_ref, load_ref,
    raw, ids_all, weights_all, partial, arrived, scale_out, scale_in, own_sum, counts, counts_in,
    local_sem, raw_send, raw_recv, ids_send, ids_recv, w_send, w_recv,
    out_send, out_recv, scale_send, scale_recv, load_sems,
):
    me = lax.axis_index("expert")
    chip, core = me // CORES, me % CORES
    other = 1 - core
    partner = {"expert": chip * CORES + other}
    tokens, width = residual_ref.shape
    fanout = ids_ref.shape[0]
    per_peer = rows_hbm.shape[1]
    held = CORES * per_peer
    local_experts = held // capacity

    def peer(step):
        return lax.rem(chip + step, chips)

    def device(step):
        return {"expert": peer(step) * CORES + core}

    barrier = pltpu.get_barrier_semaphore()
    pl.semaphore_signal(barrier, inc=1, device_id=partner)
    for step in range(1, chips):
        pl.semaphore_signal(barrier, inc=1, device_id=device(step))

    local = []
    for j in range(chips):
        copy = pltpu.make_async_copy(rows_hbm.at[j * CORES + core], raw.at[j, core], local_sem.at[j])
        copy.start()
        local.append(copy)
    pl.semaphore_wait(barrier, chips)

    routing = []
    for step in range(1, chips):
        a = pltpu.make_async_remote_copy(
            ids_ref, ids_all.at[step], ids_send.at[step], ids_recv.at[step], device_id=device(step))
        b = pltpu.make_async_remote_copy(
            weights_ref, weights_all.at[step], w_send.at[step], w_recv.at[step], device_id=device(step))
        a.start()
        b.start()
        routing.append((a, b))
    rows = []
    for j in range(chips):
        copy = pltpu.make_async_remote_copy(
            rows_hbm.at[j * CORES + other], raw.at[j, core], raw_send.at[j], raw_recv.at[j],
            device_id=partner)
        copy.start()
        rows.append(copy)

    before = (lax.broadcasted_iota(jnp.int32, (tokens, tokens), 0)
              < lax.broadcasted_iota(jnp.int32, (tokens, tokens), 1)).astype(jnp.float32).astype(jnp.bfloat16)
    place = lax.broadcasted_iota(jnp.int32, (held, local_experts), 0)
    which = lax.broadcasted_iota(jnp.int32, (held, local_experts), 1)
    low = which * capacity
    spread = ((place >= low) & (place < low + capacity)).astype(jnp.float32).astype(jnp.bfloat16)
    wanted = (lax.broadcasted_iota(jnp.int32, (held, tokens), 0) % capacity).astype(jnp.float32)
    expert = lax.broadcasted_iota(jnp.int32, (local_experts, tokens), 0) + chip * local_experts

    def select(ids, weights):
        chosen = jnp.zeros((local_experts, tokens), jnp.float32)
        weight = jnp.zeros((local_experts, tokens), jnp.float32)
        for k in range(fanout):
            hit = ids[k:k + 1, :] == expert
            chosen = jnp.where(hit, 1.0, chosen)
            weight = jnp.where(hit, weights[k:k + 1, :], weight)
        slot = dot(chosen.astype(jnp.bfloat16), before)
        slot = jnp.where(chosen > 0, slot, -1.0)
        keep = dot(spread, slot.astype(jnp.bfloat16)) == wanted
        pieces = []
        rest = weight
        for _ in range(3):
            piece = rest.astype(jnp.bfloat16)
            rest = rest - piece.astype(jnp.float32)
            pieces.append(jnp.where(keep, dot(spread, piece), 0.0))
        return pieces

    def combine(pieces, block):
        total = None
        for piece in pieces:
            part = dot(jnp.transpose(piece).astype(jnp.bfloat16), block)
            total = part if total is None else total + part
        return total

    sends = []
    order = [chips // 2] + [s for s in range(1, chips) if s != chips // 2]
    for j in range(chips):
        local[j].wait()
        rows[j].wait()
    for step in order:
        routing[step - 1][0].wait()
        routing[step - 1][1].wait()
        j = lax.rem(chip + chips - step, chips)
        pieces = select(ids_all[step], weights_all[step])
        code, scale = encode(combine(pieces, raw[j].reshape(held, width)))
        partial[step] = code
        scale_out[step] = scale
        small = pltpu.make_async_remote_copy(
            scale_out.at[step], scale_in.at[step], scale_send.at[step], scale_recv.at[step],
            device_id=device(chips - step))
        small.start()
        copy = pltpu.make_async_remote_copy(
            partial.at[step], arrived.at[step], out_send.at[step], out_recv.at[step],
            device_id=device(chips - step))
        copy.start()
        sends.append((small, copy))

    own_sum[...] = combine(select(ids_ref[...], weights_ref[...]), raw[chip].reshape(held, width))

    every = lax.broadcasted_iota(jnp.int32, (EXPERTS, tokens), 0)
    seen = jnp.zeros((EXPERTS, tokens), jnp.float32)
    for step in range(chips):
        ids = ids_ref[...] if step == 0 else ids_all[step]
        for k in range(fanout):
            seen = seen + jnp.where(ids[k:k + 1, :] == every, 1.0, 0.0)
    ones = jnp.ones((8, tokens), jnp.float32).astype(jnp.bfloat16)
    counts[...] = dot(ones, seen.astype(jnp.bfloat16), (((1,), (1,)), ((), ())))
    tally = pltpu.make_async_remote_copy(
        counts, counts_in, load_sems.at[0], load_sems.at[1], device_id=partner)
    tally.start()

    own_sum[...] = own_sum[...] + residual_ref[...].astype(jnp.float32)
    tally.wait()
    load_ref[...] = (counts[...] + counts_in[...])[0:1, :]
    for n, step in enumerate(order):
        sends[n][0].wait()
        sends[n][1].wait()
        own_sum[...] = own_sum[...] + decode(arrived[step], scale_in[step])
    mixed_ref[...] = own_sum[...].astype(jnp.bfloat16)


def fused(chips, residual, expert_ids, route_weights, expert_out):
    peers = chips * CORES
    tokens, width = residual.shape
    fanout = expert_ids.shape[1]
    per_peer = expert_out.shape[0] // peers
    capacity = expert_out.shape[0] // EXPERTS
    vmem = pl.BlockSpec(memory_space=pltpu.VMEM)
    dma = pltpu.SemaphoreType.DMA
    mixed, load = pl.pallas_call(
        functools.partial(combine_kernel, chips, capacity),
        out_shape=(
            jax.ShapeDtypeStruct((tokens, width), jnp.bfloat16),
            jax.ShapeDtypeStruct((1, EXPERTS), jnp.float32),
        ),
        in_specs=[vmem, vmem, vmem, pl.BlockSpec(memory_space=pl.ANY)],
        out_specs=(vmem, vmem),
        scratch_shapes=[
            pltpu.VMEM((chips, CORES, per_peer, width), jnp.bfloat16),
            pltpu.VMEM((chips, fanout, tokens), jnp.int32),
            pltpu.VMEM((chips, fanout, tokens), jnp.float32),
            pltpu.VMEM((chips, tokens, width), jnp.int16),
            pltpu.VMEM((chips, tokens, width), jnp.int16),
            pltpu.VMEM((chips, 8, tokens), jnp.float32),
            pltpu.VMEM((chips, 8, tokens), jnp.float32),
            pltpu.VMEM((tokens, width), jnp.float32),
            pltpu.VMEM((8, EXPERTS), jnp.float32),
            pltpu.VMEM((8, EXPERTS), jnp.float32),
        ] + [dma((chips,))] * 11 + [dma((2,))],
        compiler_params=pltpu.CompilerParams(collective_id=0, has_side_effects=True),
    )(expert_ids.T, route_weights.T, residual, expert_out.reshape(peers, per_peer, width))
    return mixed, load.reshape(EXPERTS)


def general(residual, expert_ids, route_weights, expert_out):
    peers = lax.axis_size("expert")
    per_peer = expert_out.shape[0] // peers
    width = residual.shape[1]
    tokens_here = expert_ids.shape[0]
    fanout = expert_ids.shape[1]
    capacity = expert_out.shape[0] // EXPERTS
    routes = expert_ids.reshape(-1)
    onehot = (routes[:, None] == jnp.arange(EXPERTS, dtype=jnp.int32)[None, :]).astype(jnp.int32)
    earlier = jnp.cumsum(onehot, axis=0, dtype=jnp.int32) - onehot
    slots = jnp.sum(earlier * onehot, axis=1, dtype=jnp.int32)
    source_rows = routes * capacity + slots
    load_totals = lax.psum(jnp.sum(onehot, axis=0).astype(jnp.float32), "expert")
    blocks = expert_out.reshape(peers, per_peer, width)
    arrived = lax.all_to_all(blocks, "expert", split_axis=0, concat_axis=0, tiled=True)
    picked = jnp.take(arrived.reshape(peers * per_peer, width), source_rows, axis=0)
    picked = picked.reshape(tokens_here, fanout, width)
    total = residual.astype(jnp.float32)
    for k in range(fanout):
        total = total + route_weights[:, k, None] * picked[:, k].astype(jnp.float32)
    return total.astype(jnp.bfloat16), load_totals


def solution(mesh):
    peers = mesh.shape["expert"]

    def per_device(residual, expert_ids, route_weights, expert_out):
        tokens, width = residual.shape
        slots = expert_out.shape[0]
        capacity, per_peer = slots // EXPERTS, slots // peers
        chips = peers // CORES
        needed = slots * width * 2 + (2 * chips + 4) * tokens * width * 4
        fits = (
            peers % CORES == 0 and chips > 1 and slots % EXPERTS == 0
            and per_peer % capacity == 0 and per_peer % 16 == 0 and needed <= VMEM_BUDGET
        )
        if fits:
            return fused(chips, residual, expert_ids, route_weights, expert_out)
        return general(residual, expert_ids, route_weights, expert_out)

    split = P(("dp", "expert"), None)
    return jax.shard_map(
        per_device,
        mesh=mesh,
        in_specs=(split,) * 4,
        out_specs=(split, P("dp")),
        check_vma=False,
    )
```

```python
import functools
import jax
import jax.numpy as jnp
from jax import lax
from jax.experimental import pallas as pl
from jax.experimental.pallas import tpu as pltpu
from jax.sharding import PartitionSpec as P

EXPERTS = 64
CORES = 2
VMEM_BUDGET = 24 * 1024 * 1024


def dot(a, b, dims=(((1,), (0,)), ((), ()))):
    return lax.dot_general(a, b, dims, preferred_element_type=jnp.float32)


LEVELS = 32767.0


def encode(x):
    top = jnp.maximum(jnp.max(jnp.abs(x), axis=1, keepdims=True), 1e-30)
    code = jnp.round(x * (LEVELS / top)).astype(jnp.int32).astype(jnp.int16)
    scale = jnp.transpose(jnp.broadcast_to(top * (1.0 / LEVELS), (x.shape[0], 128)))[0:8, :]
    return code, scale


def decode(code, scale):
    column = jnp.transpose(jnp.broadcast_to(scale[0:1, :], (128, scale.shape[1])))[:, 0:1]
    return code.astype(jnp.int32).astype(jnp.float32) * column


def combine_kernel(
    chips, capacity,
    ids_ref, weights_ref, residual_ref, rows_hbm,
    mixed_ref, load_ref,
    raw, ids_all, weights_all, partial, arrived, scale_out, scale_in, own_sum, counts, counts_in,
    local_sem, raw_send, raw_recv, ids_send, ids_recv, w_send, w_recv,
    out_send, out_recv, scale_send, scale_recv, load_sems,
):
    me = lax.axis_index("expert")
    chip, core = me // CORES, me % CORES
    other = 1 - core
    partner = {"expert": chip * CORES + other}
    tokens, width = residual_ref.shape
    fanout = ids_ref.shape[0]
    per_peer = rows_hbm.shape[1]
    held = CORES * per_peer
    local_experts = held // capacity

    relayed = chips >= 4
    last = chips - 1
    at_end = (chip == 0) | (chip == last)
    relays = (chip == 1) | (chip == last - 1)
    far_end = last - chip
    inner = jnp.where(chip == 0, 1, last - 1)

    def by_chip(values):
        out = jnp.int32(values[0])
        for c in range(1, chips):
            out = jnp.where(chip == c, values[c], out)
        return out

    def ordered(c):
        others = [j for j in range(chips) if j != c]
        middle = (chips - 1) / 2
        if c in (0, chips - 1):
            return sorted(others, key=lambda j: -abs(j - c))
        return sorted(others, key=lambda j: (abs(j - c), abs(j - middle)))

    tables = [ordered(c) for c in range(chips)]
    targets = [by_chip([tables[c][n] for c in range(chips)]) for n in range(chips - 1)]

    def device(j):
        return {"expert": j * CORES + core}

    def peer(step):
        return lax.rem(chip + step, chips)

    barrier = pltpu.get_barrier_semaphore()
    pl.semaphore_signal(barrier, inc=1, device_id=partner)
    for step in range(1, chips):
        pl.semaphore_signal(barrier, inc=1, device_id=device(peer(step)))

    local = []
    for j in range(chips):
        copy = pltpu.make_async_copy(rows_hbm.at[j * CORES + core], raw.at[j, core], local_sem.at[j])
        copy.start()
        local.append(copy)
    pl.semaphore_wait(barrier, chips)

    def routing(slot, j):
        return (
            pltpu.make_async_remote_copy(
                ids_ref, ids_all.at[slot], ids_send.at[j], ids_recv.at[slot], device_id=device(j)),
            pltpu.make_async_remote_copy(
                weights_ref, weights_all.at[slot], w_send.at[j], w_recv.at[slot], device_id=device(j)),
        )

    for step in range(1, chips):
        for copy in routing(chip, peer(step)):
            copy.start()
    rows = []
    for j in range(chips):
        copy = pltpu.make_async_remote_copy(
            rows_hbm.at[j * CORES + other], raw.at[j, core], raw_send.at[j], raw_recv.at[j],
            device_id=partner)
        copy.start()
        rows.append(copy)

    before = (lax.broadcasted_iota(jnp.int32, (tokens, tokens), 0)
              < lax.broadcasted_iota(jnp.int32, (tokens, tokens), 1)).astype(jnp.float32).astype(jnp.bfloat16)
    place = lax.broadcasted_iota(jnp.int32, (held, local_experts), 0)
    which = lax.broadcasted_iota(jnp.int32, (held, local_experts), 1)
    low = which * capacity
    spread = ((place >= low) & (place < low + capacity)).astype(jnp.float32).astype(jnp.bfloat16)
    wanted = (lax.broadcasted_iota(jnp.int32, (held, tokens), 0) % capacity).astype(jnp.float32)
    expert = lax.broadcasted_iota(jnp.int32, (local_experts, tokens), 0) + chip * local_experts

    def select(ids, weights):
        chosen = jnp.zeros((local_experts, tokens), jnp.float32)
        weight = jnp.zeros((local_experts, tokens), jnp.float32)
        for k in range(fanout):
            hit = ids[k:k + 1, :] == expert
            chosen = jnp.where(hit, 1.0, chosen)
            weight = jnp.where(hit, weights[k:k + 1, :], weight)
        slot = dot(chosen.astype(jnp.bfloat16), before)
        slot = jnp.where(chosen > 0, slot, -1.0)
        keep = dot(spread, slot.astype(jnp.bfloat16)) == wanted
        pieces = []
        rest = weight
        for _ in range(3):
            piece = rest.astype(jnp.bfloat16)
            rest = rest - piece.astype(jnp.float32)
            pieces.append(jnp.where(keep, dot(spread, piece), 0.0))
        return pieces

    def combine(pieces, block):
        total = None
        for piece in pieces:
            part = dot(jnp.transpose(piece).astype(jnp.bfloat16), block)
            total = part if total is None else total + part
        return total

    def message(source, slot, to):
        return (
            pltpu.make_async_remote_copy(
                scale_out.at[source], scale_in.at[slot], scale_send.at[source], scale_recv.at[slot],
                device_id=device(to)),
            pltpu.make_async_remote_copy(
                partial.at[source], arrived.at[slot], out_send.at[source], out_recv.at[slot],
                device_id=device(to)),
        )

    def take(slot):
        for copy in message(0, slot, peer(1)):
            copy.wait_recv()
        return decode(arrived[slot], scale_in[slot])

    for j in range(chips):
        local[j].wait()
        rows[j].wait()
    for n, j in enumerate(targets):
        for copy in routing(j, j):
            copy.wait_recv()
        value = combine(select(ids_all[j], weights_all[j]), raw[j].reshape(held, width))
        if relayed and n == chips - 2:
            own_sum[...] = value

            @pl.when(relays)
            def _():
                own_sum[...] = own_sum[...] + take(chips)

            value = own_sum[...]
        partial[n], scale_out[n] = encode(value)
        to, slot = j, chip
        if relayed and n == 0:
            to, slot = jnp.where(at_end, inner, j), jnp.where(at_end, chips, chip)
        for copy in message(n, slot, to):
            copy.start()

    own_sum[...] = combine(select(ids_ref[...], weights_ref[...]), raw[chip].reshape(held, width))
    own_sum[...] = own_sum[...] + residual_ref[...].astype(jnp.float32)

    every = lax.broadcasted_iota(jnp.int32, (EXPERTS, tokens), 0)
    seen = jnp.zeros((EXPERTS, tokens), jnp.float32)
    for step in range(chips):
        ids = ids_ref[...] if step == 0 else ids_all[peer(step)]
        for k in range(fanout):
            seen = seen + jnp.where(ids[k:k + 1, :] == every, 1.0, 0.0)
    ones = jnp.ones((8, tokens), jnp.float32).astype(jnp.bfloat16)
    counts[...] = dot(ones, seen.astype(jnp.bfloat16), (((1,), (1,)), ((), ())))
    tally = pltpu.make_async_remote_copy(
        counts, counts_in, load_sems.at[0], load_sems.at[1], device_id=partner)
    tally.start()
    tally.wait()
    load_ref[...] = (counts[...] + counts_in[...])[0:1, :]

    for s in targets:
        if relayed:
            @pl.when(jnp.logical_not(at_end & (s == far_end)))
            def _():
                own_sum[...] = own_sum[...] + take(s)
        else:
            own_sum[...] = own_sum[...] + take(s)
    mixed_ref[...] = own_sum[...].astype(jnp.bfloat16)

    for step in range(1, chips):
        for copy in routing(chip, peer(step)):
            copy.wait_send()
    for n in range(chips - 1):
        for copy in message(n, n, peer(1)):
            copy.wait_send()


def write_kernel(mixed_ref, load_ref, mixed_out, load_out, sems):
    first = pltpu.make_async_copy(mixed_ref, mixed_out, sems.at[0])
    second = pltpu.make_async_copy(load_ref, load_out, sems.at[1])
    first.start()
    second.start()
    first.wait()
    second.wait()


def fused(chips, residual, expert_ids, route_weights, expert_out):
    peers = chips * CORES
    tokens, width = residual.shape
    fanout = expert_ids.shape[1]
    per_peer = expert_out.shape[0] // peers
    capacity = expert_out.shape[0] // EXPERTS
    vmem = pl.BlockSpec(memory_space=pltpu.VMEM)
    hbm = pl.BlockSpec(memory_space=pl.ANY)
    dma = pltpu.SemaphoreType.DMA
    shapes = (
        jax.ShapeDtypeStruct((tokens, width), jnp.bfloat16),
        jax.ShapeDtypeStruct((1, EXPERTS), jnp.float32),
    )
    slots = chips + 1
    results = pl.pallas_call(
        functools.partial(combine_kernel, chips, capacity),
        out_shape=shapes,
        in_specs=[vmem, vmem, vmem, hbm],
        out_specs=(vmem, vmem),
        scratch_shapes=[
            pltpu.VMEM((chips, CORES, per_peer, width), jnp.bfloat16),
            pltpu.VMEM((chips, fanout, tokens), jnp.int32),
            pltpu.VMEM((chips, fanout, tokens), jnp.float32),
            pltpu.VMEM((chips, tokens, width), jnp.int16),
            pltpu.VMEM((slots, tokens, width), jnp.int16),
            pltpu.VMEM((chips, 8, tokens), jnp.float32),
            pltpu.VMEM((slots, 8, tokens), jnp.float32),
            pltpu.VMEM((tokens, width), jnp.float32),
            pltpu.VMEM((8, EXPERTS), jnp.float32),
            pltpu.VMEM((8, EXPERTS), jnp.float32),
        ] + [dma((slots,))] * 11 + [dma((2,))],
        compiler_params=pltpu.CompilerParams(collective_id=0, has_side_effects=True),
    )(expert_ids.T, route_weights.T, residual, expert_out.reshape(peers, per_peer, width))
    mixed, load = pl.pallas_call(
        write_kernel,
        out_shape=shapes,
        in_specs=[vmem, vmem],
        out_specs=(hbm, hbm),
        scratch_shapes=[dma((2,))],
    )(*results)
    return mixed, load.reshape(EXPERTS)


def general(residual, expert_ids, route_weights, expert_out):
    peers = lax.axis_size("expert")
    per_peer = expert_out.shape[0] // peers
    width = residual.shape[1]
    tokens_here = expert_ids.shape[0]
    fanout = expert_ids.shape[1]
    capacity = expert_out.shape[0] // EXPERTS
    routes = expert_ids.reshape(-1)
    onehot = (routes[:, None] == jnp.arange(EXPERTS, dtype=jnp.int32)[None, :]).astype(jnp.int32)
    earlier = jnp.cumsum(onehot, axis=0, dtype=jnp.int32) - onehot
    slots = jnp.sum(earlier * onehot, axis=1, dtype=jnp.int32)
    source_rows = routes * capacity + slots
    load_totals = lax.psum(jnp.sum(onehot, axis=0).astype(jnp.float32), "expert")
    blocks = expert_out.reshape(peers, per_peer, width)
    arrived = lax.all_to_all(blocks, "expert", split_axis=0, concat_axis=0, tiled=True)
    picked = jnp.take(arrived.reshape(peers * per_peer, width), source_rows, axis=0)
    picked = picked.reshape(tokens_here, fanout, width)
    total = residual.astype(jnp.float32)
    for k in range(fanout):
        total = total + route_weights[:, k, None] * picked[:, k].astype(jnp.float32)
    return total.astype(jnp.bfloat16), load_totals


def solution(mesh):
    peers = mesh.shape["expert"]

    def per_device(residual, expert_ids, route_weights, expert_out):
        tokens, width = residual.shape
        slots = expert_out.shape[0]
        capacity, per_peer = slots // EXPERTS, slots // peers
        chips = peers // CORES
        needed = slots * width * 2 + (2 * chips + 4) * tokens * width * 4
        fits = (
            peers % CORES == 0 and chips > 1 and slots % EXPERTS == 0
            and per_peer % capacity == 0 and per_peer % 16 == 0 and needed <= VMEM_BUDGET
        )
        if fits:
            return fused(chips, residual, expert_ids, route_weights, expert_out)
        return general(residual, expert_ids, route_weights, expert_out)

    split = P(("dp", "expert"), None)
    return jax.shard_map(
        per_device,
        mesh=mesh,
        in_specs=(split,) * 4,
        out_specs=(split, P("dp")),
        check_vma=False,
    )
```

```python
import functools
import jax
import jax.numpy as jnp
from jax import lax
from jax.experimental import pallas as pl
from jax.experimental.pallas import tpu as pltpu
from jax.sharding import PartitionSpec as P

EXPERTS = 64
CORES = 2
VMEM_BUDGET = 24 * 1024 * 1024


def dot(a, b, dims=(((1,), (0,)), ((), ()))):
    return lax.dot_general(a, b, dims, preferred_element_type=jnp.float32)


LEVELS = 32767.0


def encode(x):
    top = jnp.maximum(jnp.max(jnp.abs(x), axis=1, keepdims=True), 1e-30)
    code = jnp.round(x * (LEVELS / top)).astype(jnp.int32).astype(jnp.int16)
    scale = jnp.transpose(jnp.broadcast_to(top * (1.0 / LEVELS), (x.shape[0], 128)))[0:8, :]
    return code, scale


def decode(code, scale):
    column = jnp.transpose(jnp.broadcast_to(scale[0:1, :], (128, scale.shape[1])))[:, 0:1]
    return code.astype(jnp.int32).astype(jnp.float32) * column


def combine_kernel(
    chips, capacity,
    ids_hbm, weights_hbm, residual_hbm, rows_hbm,
    mixed_ref, load_ref,
    ids_ref, weights_ref, residual_ref, raw, ids_all, weights_all, partial, arrived, scale_out, scale_in, own_sum, counts, counts_in,
    local_sem, raw_send, raw_recv, ids_send, ids_recv, w_send, w_recv,
    out_send, out_recv, scale_send, scale_recv, load_sems, in_sems,
):
    me = lax.axis_index("expert")
    chip, core = me // CORES, me % CORES
    other = 1 - core
    partner = {"expert": chip * CORES + other}
    tokens, width = residual_ref.shape
    fanout = ids_ref.shape[0]
    per_peer = rows_hbm.shape[1]
    held = CORES * per_peer
    local_experts = held // capacity

    relayed = chips >= 4
    last = chips - 1
    at_end = (chip == 0) | (chip == last)
    relays = (chip == 1) | (chip == last - 1)
    far_end = last - chip
    inner = jnp.where(chip == 0, 1, last - 1)

    def by_chip(values):
        out = jnp.int32(values[0])
        for c in range(1, chips):
            out = jnp.where(chip == c, values[c], out)
        return out

    def ordered(c):
        others = [j for j in range(chips) if j != c]
        middle = (chips - 1) / 2
        if c in (0, chips - 1):
            return sorted(others, key=lambda j: -abs(j - c))
        return sorted(others, key=lambda j: (abs(j - c), abs(j - middle)))

    tables = [ordered(c) for c in range(chips)]
    targets = [by_chip([tables[c][n] for c in range(chips)]) for n in range(chips - 1)]

    def device(j):
        return {"expert": j * CORES + core}

    def peer(step):
        return lax.rem(chip + step, chips)

    barrier = pltpu.get_barrier_semaphore()
    pl.semaphore_signal(barrier, inc=1, device_id=partner)
    for step in range(1, chips):
        pl.semaphore_signal(barrier, inc=1, device_id=device(peer(step)))

    fetched = []
    for n, (source, target) in enumerate(
            ((ids_hbm, ids_ref), (weights_hbm, weights_ref), (residual_hbm, residual_ref))):
        copy = pltpu.make_async_copy(source, target, in_sems.at[n])
        copy.start()
        fetched.append(copy)
    local = []
    for j in range(chips):
        copy = pltpu.make_async_copy(rows_hbm.at[j * CORES + core], raw.at[j, core], local_sem.at[j])
        copy.start()
        local.append(copy)
    fetched[0].wait()
    fetched[1].wait()
    pl.semaphore_wait(barrier, chips)

    def routing(slot, j):
        return (
            pltpu.make_async_remote_copy(
                ids_ref, ids_all.at[slot], ids_send.at[j], ids_recv.at[slot], device_id=device(j)),
            pltpu.make_async_remote_copy(
                weights_ref, weights_all.at[slot], w_send.at[j], w_recv.at[slot], device_id=device(j)),
        )

    for step in range(1, chips):
        for copy in routing(chip, peer(step)):
            copy.start()
    rows = []
    for j in range(chips):
        copy = pltpu.make_async_remote_copy(
            rows_hbm.at[j * CORES + other], raw.at[j, core], raw_send.at[j], raw_recv.at[j],
            device_id=partner)
        copy.start()
        rows.append(copy)

    before = (lax.broadcasted_iota(jnp.int32, (tokens, tokens), 0)
              < lax.broadcasted_iota(jnp.int32, (tokens, tokens), 1)).astype(jnp.float32).astype(jnp.bfloat16)
    place = lax.broadcasted_iota(jnp.int32, (held, local_experts), 0)
    which = lax.broadcasted_iota(jnp.int32, (held, local_experts), 1)
    low = which * capacity
    spread = ((place >= low) & (place < low + capacity)).astype(jnp.float32).astype(jnp.bfloat16)
    wanted = (lax.broadcasted_iota(jnp.int32, (held, tokens), 0) % capacity).astype(jnp.float32)
    expert = lax.broadcasted_iota(jnp.int32, (local_experts, tokens), 0) + chip * local_experts

    def select(ids, weights):
        chosen = jnp.zeros((local_experts, tokens), jnp.float32)
        weight = jnp.zeros((local_experts, tokens), jnp.float32)
        for k in range(fanout):
            hit = ids[k:k + 1, :] == expert
            chosen = jnp.where(hit, 1.0, chosen)
            weight = jnp.where(hit, weights[k:k + 1, :], weight)
        slot = dot(chosen.astype(jnp.bfloat16), before)
        slot = jnp.where(chosen > 0, slot, -1.0)
        keep = dot(spread, slot.astype(jnp.bfloat16)) == wanted
        pieces = []
        rest = weight
        for _ in range(3):
            piece = rest.astype(jnp.bfloat16)
            rest = rest - piece.astype(jnp.float32)
            pieces.append(jnp.where(keep, dot(spread, piece), 0.0))
        return pieces

    def combine(pieces, block):
        total = None
        for piece in pieces:
            part = dot(jnp.transpose(piece).astype(jnp.bfloat16), block)
            total = part if total is None else total + part
        return total

    def message(source, slot, to):
        return (
            pltpu.make_async_remote_copy(
                scale_out.at[source], scale_in.at[slot], scale_send.at[source], scale_recv.at[slot],
                device_id=device(to)),
            pltpu.make_async_remote_copy(
                partial.at[source], arrived.at[slot], out_send.at[source], out_recv.at[slot],
                device_id=device(to)),
        )

    def take(slot):
        for copy in message(0, slot, peer(1)):
            copy.wait_recv()
        return decode(arrived[slot], scale_in[slot])

    for j in range(chips):
        local[j].wait()
        rows[j].wait()
    for n, j in enumerate(targets):
        for copy in routing(j, j):
            copy.wait_recv()
        value = combine(select(ids_all[j], weights_all[j]), raw[j].reshape(held, width))
        if relayed and n == chips - 2:
            own_sum[...] = value

            @pl.when(relays)
            def _():
                own_sum[...] = own_sum[...] + take(chips)

            value = own_sum[...]
        partial[n], scale_out[n] = encode(value)
        to, slot = j, chip
        if relayed and n == 0:
            to, slot = jnp.where(at_end, inner, j), jnp.where(at_end, chips, chip)
        for copy in message(n, slot, to):
            copy.start()

    own_sum[...] = combine(select(ids_ref[...], weights_ref[...]), raw[chip].reshape(held, width))
    fetched[2].wait()
    own_sum[...] = own_sum[...] + residual_ref[...].astype(jnp.float32)

    every = lax.broadcasted_iota(jnp.int32, (EXPERTS, tokens), 0)
    seen = jnp.zeros((EXPERTS, tokens), jnp.float32)
    for step in range(chips):
        ids = ids_ref[...] if step == 0 else ids_all[peer(step)]
        for k in range(fanout):
            seen = seen + jnp.where(ids[k:k + 1, :] == every, 1.0, 0.0)
    ones = jnp.ones((8, tokens), jnp.float32).astype(jnp.bfloat16)
    counts[...] = dot(ones, seen.astype(jnp.bfloat16), (((1,), (1,)), ((), ())))
    tally = pltpu.make_async_remote_copy(
        counts, counts_in, load_sems.at[0], load_sems.at[1], device_id=partner)
    tally.start()
    tally.wait()
    load_ref[...] = (counts[...] + counts_in[...])[0:1, :]

    for s in targets:
        if relayed:
            @pl.when(jnp.logical_not(at_end & (s == far_end)))
            def _():
                own_sum[...] = own_sum[...] + take(s)
        else:
            own_sum[...] = own_sum[...] + take(s)
    mixed_ref[...] = own_sum[...].astype(jnp.bfloat16)

    for step in range(1, chips):
        for copy in routing(chip, peer(step)):
            copy.wait_send()
    for n in range(chips - 1):
        for copy in message(n, n, peer(1)):
            copy.wait_send()


def write_kernel(mixed_ref, load_ref, mixed_out, load_out, sems):
    first = pltpu.make_async_copy(mixed_ref, mixed_out, sems.at[0])
    second = pltpu.make_async_copy(load_ref, load_out, sems.at[1])
    first.start()
    second.start()
    first.wait()
    second.wait()


def fused(chips, residual, expert_ids, route_weights, expert_out):
    peers = chips * CORES
    tokens, width = residual.shape
    fanout = expert_ids.shape[1]
    per_peer = expert_out.shape[0] // peers
    capacity = expert_out.shape[0] // EXPERTS
    vmem = pl.BlockSpec(memory_space=pltpu.VMEM)
    hbm = pl.BlockSpec(memory_space=pl.ANY)
    dma = pltpu.SemaphoreType.DMA
    shapes = (
        jax.ShapeDtypeStruct((tokens, width), jnp.bfloat16),
        jax.ShapeDtypeStruct((1, EXPERTS), jnp.float32),
    )
    slots = chips + 1
    results = pl.pallas_call(
        functools.partial(combine_kernel, chips, capacity),
        out_shape=tuple(pltpu.VMEM(x.shape, x.dtype) for x in shapes),
        in_specs=[hbm, hbm, hbm, hbm],
        out_specs=(vmem, vmem),
        scratch_shapes=[
            pltpu.VMEM((fanout, tokens), jnp.int32),
            pltpu.VMEM((fanout, tokens), jnp.float32),
            pltpu.VMEM((tokens, width), jnp.bfloat16),
            pltpu.VMEM((chips, CORES, per_peer, width), jnp.bfloat16),
            pltpu.VMEM((chips, fanout, tokens), jnp.int32),
            pltpu.VMEM((chips, fanout, tokens), jnp.float32),
            pltpu.VMEM((chips, tokens, width), jnp.int16),
            pltpu.VMEM((slots, tokens, width), jnp.int16),
            pltpu.VMEM((chips, 8, tokens), jnp.float32),
            pltpu.VMEM((slots, 8, tokens), jnp.float32),
            pltpu.VMEM((tokens, width), jnp.float32),
            pltpu.VMEM((8, EXPERTS), jnp.float32),
            pltpu.VMEM((8, EXPERTS), jnp.float32),
        ] + [dma((slots,))] * 11 + [dma((2,)), dma((3,))],
        compiler_params=pltpu.CompilerParams(collective_id=0, has_side_effects=True),
    )(expert_ids.T, route_weights.T, residual, expert_out.reshape(peers, per_peer, width))
    mixed, load = pl.pallas_call(
        write_kernel,
        out_shape=shapes,
        in_specs=[vmem, vmem],
        out_specs=(hbm, hbm),
        scratch_shapes=[dma((2,))],
    )(*[pltpu.with_memory_space_constraint(x, pltpu.VMEM) for x in results])
    return mixed, load.reshape(EXPERTS)


def general(residual, expert_ids, route_weights, expert_out):
    peers = lax.axis_size("expert")
    per_peer = expert_out.shape[0] // peers
    width = residual.shape[1]
    tokens_here = expert_ids.shape[0]
    fanout = expert_ids.shape[1]
    capacity = expert_out.shape[0] // EXPERTS
    routes = expert_ids.reshape(-1)
    onehot = (routes[:, None] == jnp.arange(EXPERTS, dtype=jnp.int32)[None, :]).astype(jnp.int32)
    earlier = jnp.cumsum(onehot, axis=0, dtype=jnp.int32) - onehot
    slots = jnp.sum(earlier * onehot, axis=1, dtype=jnp.int32)
    source_rows = routes * capacity + slots
    load_totals = lax.psum(jnp.sum(onehot, axis=0).astype(jnp.float32), "expert")
    blocks = expert_out.reshape(peers, per_peer, width)
    arrived = lax.all_to_all(blocks, "expert", split_axis=0, concat_axis=0, tiled=True)
    picked = jnp.take(arrived.reshape(peers * per_peer, width), source_rows, axis=0)
    picked = picked.reshape(tokens_here, fanout, width)
    total = residual.astype(jnp.float32)
    for k in range(fanout):
        total = total + route_weights[:, k, None] * picked[:, k].astype(jnp.float32)
    return total.astype(jnp.bfloat16), load_totals


def solution(mesh):
    peers = mesh.shape["expert"]

    def per_device(residual, expert_ids, route_weights, expert_out):
        tokens, width = residual.shape
        slots = expert_out.shape[0]
        capacity, per_peer = slots // EXPERTS, slots // peers
        chips = peers // CORES
        needed = slots * width * 2 + (2 * chips + 4) * tokens * width * 4
        fits = (
            peers % CORES == 0 and chips > 1 and slots % EXPERTS == 0
            and per_peer % capacity == 0 and per_peer % 16 == 0 and needed <= VMEM_BUDGET
        )
        if fits:
            return fused(chips, residual, expert_ids, route_weights, expert_out)
        return general(residual, expert_ids, route_weights, expert_out)

    split = P(("dp", "expert"), None)
    return jax.shard_map(
        per_device,
        mesh=mesh,
        in_specs=(split,) * 4,
        out_specs=(split, P("dp")),
        check_vma=False,
    )
```

```python
import functools
import jax
import jax.numpy as jnp
from jax import lax
from jax.experimental import pallas as pl
from jax.experimental.pallas import tpu as pltpu
from jax.sharding import PartitionSpec as P

EXPERTS = 64
CORES = 2
VMEM_BUDGET = 24 * 1024 * 1024


def dot(a, b, dims=(((1,), (0,)), ((), ()))):
    return lax.dot_general(a, b, dims, preferred_element_type=jnp.float32)


LEVELS = 32767.0
PARTS = 2
RELAY_TURN = 0


def encode(x):
    top = jnp.maximum(jnp.max(jnp.abs(x), axis=1, keepdims=True), 1e-30)
    code = jnp.round(x * (LEVELS / top)).astype(jnp.int32).astype(jnp.int16)
    scale = jnp.transpose(jnp.broadcast_to(top * (1.0 / LEVELS), (x.shape[0], 128)))[0:8, :]
    return code, scale


def decode(code, scale):
    column = jnp.transpose(jnp.broadcast_to(scale[0:1, :], (128, scale.shape[1])))[:, 0:1]
    return code.astype(jnp.int32).astype(jnp.float32) * column


def combine_kernel(
    chips, capacity,
    ids_hbm, weights_hbm, residual_hbm, rows_hbm,
    mixed_ref, load_ref,
    ids_ref, weights_ref, residual_ref, staged, raw, ids_all, weights_all, partial, arrived, scale_out, scale_in, own_sum, counts, counts_in,
    local_sem, raw_send, raw_recv, ids_send, ids_recv, w_send, w_recv,
    out_send, out_recv, scale_send, scale_recv, stage_sems, load_sems, in_sems,
):
    me = lax.axis_index("expert")
    chip, core = me // CORES, me % CORES
    other = 1 - core
    partner = {"expert": chip * CORES + other}
    tokens, width = residual_ref.shape
    fanout = ids_ref.shape[0]
    per_peer = rows_hbm.shape[1]
    held = CORES * per_peer
    local_experts = held // capacity

    relayed = chips >= 4
    last = chips - 1
    at_end = (chip == 0) | (chip == last)
    relays = (chip == 1) | (chip == last - 1)
    far_end = last - chip
    inner = jnp.where(chip == 0, 1, last - 1)

    def by_chip(values):
        out = jnp.int32(values[0])
        for c in range(1, chips):
            out = jnp.where(chip == c, values[c], out)
        return out

    def ordered(c):
        others = [j for j in range(chips) if j != c]
        middle = (chips - 1) / 2
        if c in (0, chips - 1):
            return sorted(others, key=lambda j: -abs(j - c))
        return sorted(others, key=lambda j: (abs(j - c), abs(j - middle)))

    tables = [ordered(c) for c in range(chips)]
    targets = [by_chip([tables[c][n] for c in range(chips)]) for n in range(chips - 1)]

    needed = targets + [chip]

    def device(j):
        return {"expert": j * CORES + core}

    def peer(step):
        return lax.rem(chip + step, chips)

    barrier = pltpu.get_barrier_semaphore()
    pl.semaphore_signal(barrier, inc=1, device_id=partner)
    for step in range(1, chips):
        pl.semaphore_signal(barrier, inc=1, device_id=device(peer(step)))

    fetched = []
    for n, (source, target) in enumerate(
            ((ids_hbm, ids_ref), (weights_hbm, weights_ref), (residual_hbm, residual_ref))):
        copy = pltpu.make_async_copy(source, target, in_sems.at[n])
        copy.start()
        fetched.append(copy)
    def outbound(n):
        j = needed[n]
        return pltpu.make_async_copy(rows_hbm.at[j * CORES + other], staged.at[n], stage_sems.at[n])

    def inbound(n):
        j = needed[n]
        return pltpu.make_async_copy(rows_hbm.at[j * CORES + core], raw.at[j, core], local_sem.at[n])

    def handed(n, slot):
        return pltpu.make_async_remote_copy(
            staged.at[n], raw.at[needed[n], slot], raw_send.at[n], raw_recv.at[n], device_id=partner)

    for n in range(chips):
        outbound(n).start()
    for n in range(chips):
        inbound(n).start()
    fetched[0].wait()
    fetched[1].wait()
    pl.semaphore_wait(barrier, chips)

    def routing(slot, j):
        return (
            pltpu.make_async_remote_copy(
                ids_ref, ids_all.at[slot], ids_send.at[j], ids_recv.at[slot], device_id=device(j)),
            pltpu.make_async_remote_copy(
                weights_ref, weights_all.at[slot], w_send.at[j], w_recv.at[slot], device_id=device(j)),
        )

    for step in range(1, chips):
        for copy in routing(chip, peer(step)):
            copy.start()
    for n in range(chips):
        outbound(n).wait()
        handed(n, core).start()

    before = (lax.broadcasted_iota(jnp.int32, (tokens, tokens), 0)
              < lax.broadcasted_iota(jnp.int32, (tokens, tokens), 1)).astype(jnp.float32).astype(jnp.bfloat16)
    place = lax.broadcasted_iota(jnp.int32, (held, local_experts), 0)
    which = lax.broadcasted_iota(jnp.int32, (held, local_experts), 1)
    low = which * capacity
    spread = ((place >= low) & (place < low + capacity)).astype(jnp.float32).astype(jnp.bfloat16)
    wanted = (lax.broadcasted_iota(jnp.int32, (held, tokens), 0) % capacity).astype(jnp.float32)
    expert = lax.broadcasted_iota(jnp.int32, (local_experts, tokens), 0) + chip * local_experts

    def select(ids, weights):
        chosen = jnp.zeros((local_experts, tokens), jnp.float32)
        weight = jnp.zeros((local_experts, tokens), jnp.float32)
        for k in range(fanout):
            hit = ids[k:k + 1, :] == expert
            chosen = jnp.where(hit, 1.0, chosen)
            weight = jnp.where(hit, weights[k:k + 1, :], weight)
        slot = dot(chosen.astype(jnp.bfloat16), before)
        slot = jnp.where(chosen > 0, slot, -1.0)
        keep = dot(spread, slot.astype(jnp.bfloat16)) == wanted
        pieces = []
        rest = weight
        for _ in range(3):
            piece = rest.astype(jnp.bfloat16)
            rest = rest - piece.astype(jnp.float32)
            pieces.append(jnp.where(keep, dot(spread, piece), 0.0))
        return pieces

    def combine(pieces, block):
        stacked = jnp.concatenate([jnp.transpose(piece) for piece in pieces], axis=0)
        parts = dot(stacked.astype(jnp.bfloat16), block)
        return parts[:tokens] + parts[tokens:2 * tokens] + parts[2 * tokens:]

    size = tokens // PARTS

    def message(source, slot, part, to):
        return (
            pltpu.make_async_remote_copy(
                scale_out.at[source, part], scale_in.at[slot, part],
                scale_send.at[source, part], scale_recv.at[slot, part], device_id=device(to)),
            pltpu.make_async_remote_copy(
                partial.at[source, part], arrived.at[slot, part],
                out_send.at[source, part], out_recv.at[slot, part], device_id=device(to)),
        )

    def take(slot, part):
        for copy in message(0, slot, part, peer(1)):
            copy.wait_recv()
        return decode(arrived[slot, part], scale_in[slot, part])

    for n, j in enumerate(targets):
        for copy in routing(j, j):
            copy.wait_recv()
        pieces = select(ids_all[j], weights_all[j])
        inbound(n).wait()
        handed(n, other).wait_recv()
        value = combine(pieces, raw[j].reshape(held, width))
        to, slot = j, chip
        if relayed and n == RELAY_TURN:
            to, slot = jnp.where(at_end, inner, j), jnp.where(at_end, chips, chip)
        adds = relayed and n == chips - 2
        if adds:
            own_sum[...] = value
        for part in range(PARTS):
            span = slice(part * size, (part + 1) * size)
            if adds:
                @pl.when(relays)
                def _():
                    own_sum[span, :] = own_sum[span, :] + take(chips, part)

                piece = own_sum[span, :]
            else:
                piece = value[span, :]
            partial[n, part], scale_out[n, part] = encode(piece)
            for copy in message(n, slot, part, to):
                copy.start()

    inbound(chips - 1).wait()
    handed(chips - 1, other).wait_recv()
    own_sum[...] = combine(select(ids_ref[...], weights_ref[...]), raw[chip].reshape(held, width))
    fetched[2].wait()
    own_sum[...] = own_sum[...] + residual_ref[...].astype(jnp.float32)

    every = lax.broadcasted_iota(jnp.int32, (EXPERTS, tokens), 0)
    seen = jnp.zeros((EXPERTS, tokens), jnp.float32)
    for step in range(chips):
        ids = ids_ref[...] if step == 0 else ids_all[peer(step)]
        for k in range(fanout):
            seen = seen + jnp.where(ids[k:k + 1, :] == every, 1.0, 0.0)
    ones = jnp.ones((8, tokens), jnp.float32).astype(jnp.bfloat16)
    counts[...] = dot(ones, seen.astype(jnp.bfloat16), (((1,), (1,)), ((), ())))
    tally = pltpu.make_async_remote_copy(
        counts, counts_in, load_sems.at[0], load_sems.at[1], device_id=partner)
    tally.start()
    tally.wait()
    load_ref[...] = (counts[...] + counts_in[...])[0:1, :]

    def add(s, part):
        span = slice(part * size, (part + 1) * size)
        own_sum[span, :] = own_sum[span, :] + take(s, part)

    for s in targets:
        for part in range(PARTS):
            if relayed:
                @pl.when(jnp.logical_not(at_end & (s == far_end)))
                def _():
                    add(s, part)
            else:
                add(s, part)
    mixed_ref[...] = own_sum[...].astype(jnp.bfloat16)

    for step in range(1, chips):
        for copy in routing(chip, peer(step)):
            copy.wait_send()
    for n in range(chips):
        handed(n, core).wait_send()
    for n in range(chips - 1):
        for part in range(PARTS):
            for copy in message(n, n, part, peer(1)):
                copy.wait_send()


def write_kernel(mixed_ref, load_ref, mixed_out, load_out, sems):
    first = pltpu.make_async_copy(mixed_ref, mixed_out, sems.at[0])
    second = pltpu.make_async_copy(load_ref, load_out, sems.at[1])
    first.start()
    second.start()
    first.wait()
    second.wait()


def fused(chips, residual, expert_ids, route_weights, expert_out):
    peers = chips * CORES
    tokens, width = residual.shape
    fanout = expert_ids.shape[1]
    per_peer = expert_out.shape[0] // peers
    capacity = expert_out.shape[0] // EXPERTS
    vmem = pl.BlockSpec(memory_space=pltpu.VMEM)
    hbm = pl.BlockSpec(memory_space=pl.ANY)
    dma = pltpu.SemaphoreType.DMA
    shapes = (
        jax.ShapeDtypeStruct((tokens, width), jnp.bfloat16),
        jax.ShapeDtypeStruct((1, EXPERTS), jnp.float32),
    )
    slots = chips + 1
    results = pl.pallas_call(
        functools.partial(combine_kernel, chips, capacity),
        out_shape=tuple(pltpu.VMEM(x.shape, x.dtype) for x in shapes),
        in_specs=[hbm, hbm, hbm, hbm],
        out_specs=(vmem, vmem),
        scratch_shapes=[
            pltpu.VMEM((fanout, tokens), jnp.int32),
            pltpu.VMEM((fanout, tokens), jnp.float32),
            pltpu.VMEM((tokens, width), jnp.bfloat16),
            pltpu.VMEM((chips, per_peer, width), jnp.bfloat16),
            pltpu.VMEM((chips, CORES, per_peer, width), jnp.bfloat16),
            pltpu.VMEM((chips, fanout, tokens), jnp.int32),
            pltpu.VMEM((chips, fanout, tokens), jnp.float32),
            pltpu.VMEM((chips, PARTS, tokens // PARTS, width), jnp.int16),
            pltpu.VMEM((slots, PARTS, tokens // PARTS, width), jnp.int16),
            pltpu.VMEM((chips, PARTS, 8, tokens // PARTS), jnp.float32),
            pltpu.VMEM((slots, PARTS, 8, tokens // PARTS), jnp.float32),
            pltpu.VMEM((tokens, width), jnp.float32),
            pltpu.VMEM((8, EXPERTS), jnp.float32),
            pltpu.VMEM((8, EXPERTS), jnp.float32),
        ] + [dma((slots,))] * 7 + [dma((slots, PARTS))] * 4 + [dma((chips,)), dma((2,)), dma((3,))],
        compiler_params=pltpu.CompilerParams(collective_id=0, has_side_effects=True),
    )(expert_ids.T, route_weights.T, residual, expert_out.reshape(peers, per_peer, width))
    mixed, load = pl.pallas_call(
        write_kernel,
        out_shape=shapes,
        in_specs=[vmem, vmem],
        out_specs=(hbm, hbm),
        scratch_shapes=[dma((2,))],
    )(*[pltpu.with_memory_space_constraint(x, pltpu.VMEM) for x in results])
    return mixed, load.reshape(EXPERTS)


def general(residual, expert_ids, route_weights, expert_out):
    peers = lax.axis_size("expert")
    per_peer = expert_out.shape[0] // peers
    width = residual.shape[1]
    tokens_here = expert_ids.shape[0]
    fanout = expert_ids.shape[1]
    capacity = expert_out.shape[0] // EXPERTS
    routes = expert_ids.reshape(-1)
    onehot = (routes[:, None] == jnp.arange(EXPERTS, dtype=jnp.int32)[None, :]).astype(jnp.int32)
    earlier = jnp.cumsum(onehot, axis=0, dtype=jnp.int32) - onehot
    slots = jnp.sum(earlier * onehot, axis=1, dtype=jnp.int32)
    source_rows = routes * capacity + slots
    load_totals = lax.psum(jnp.sum(onehot, axis=0).astype(jnp.float32), "expert")
    blocks = expert_out.reshape(peers, per_peer, width)
    arrived = lax.all_to_all(blocks, "expert", split_axis=0, concat_axis=0, tiled=True)
    picked = jnp.take(arrived.reshape(peers * per_peer, width), source_rows, axis=0)
    picked = picked.reshape(tokens_here, fanout, width)
    total = residual.astype(jnp.float32)
    for k in range(fanout):
        total = total + route_weights[:, k, None] * picked[:, k].astype(jnp.float32)
    return total.astype(jnp.bfloat16), load_totals


def solution(mesh):
    peers = mesh.shape["expert"]

    def per_device(residual, expert_ids, route_weights, expert_out):
        tokens, width = residual.shape
        slots = expert_out.shape[0]
        capacity, per_peer = slots // EXPERTS, slots // peers
        chips = peers // CORES
        needed = 2 * slots * width * 2 + (2 * chips + 4) * tokens * width * 4
        fits = (
            peers % CORES == 0 and chips > 1 and slots % EXPERTS == 0
            and per_peer % capacity == 0 and per_peer % 16 == 0 and tokens % (16 * PARTS) == 0 and needed <= VMEM_BUDGET
        )
        if fits:
            return fused(chips, residual, expert_ids, route_weights, expert_out)
        return general(residual, expert_ids, route_weights, expert_out)

    split = P(("dp", "expert"), None)
    return jax.shard_map(
        per_device,
        mesh=mesh,
        in_specs=(split,) * 4,
        out_specs=(split, P("dp")),
        check_vma=False,
    )
```
